32 devices in a mesh: dp: 16 (over z, y, core), expert: 2 (over x).
Axes of the slice: x: 2, y: 2, z: 4, core: 2. Of those that a mesh axis runs over, the one named last changes fastest.
Arguments:
- tokens: bfloat16 [256, 6144], P(('dp', 'expert')), may hold values from -6 to 6
- router_now: float32 [6144, 8], P('dp'), may hold values from -0.078125 to 0.078125
- router_next: float32 [6144, 8], P('dp'), may hold values from -0.078125 to 0.078125
- w_gate: bfloat16 [8, 6144, 8192], P('expert', None, 'dp'), may hold values from -0.078125 to 0.078125
- w_up: bfloat16 [8, 6144, 8192], P('expert', None, 'dp'), may hold values from -0.078125 to 0.078125
- w_down: bfloat16 [8, 8192, 6144], P('expert', 'dp'), may hold values from -0.0625 to 0.0625
- expert_ids: int32 [256, 2], P(('dp', 'expert')), may hold values from 0 to 7, all different within a row; in each aligned block of 8 rows (0 to 7, 8 to 15, ...) at most 4 rows name the same one
- next_ids: int32 [256, 2], P(('dp', 'expert')), may hold values from 0 to 7, all different within a row
Outputs:
- layer_out: bfloat16 [256, 6144], P(('dp', 'expert'))
- next_logits: float32 [256, 8], P(('dp', 'expert'))
- next_weights: float32 [256, 2], P(('dp', 'expert'))
The draws below stay inside these ranges and needn't reach their ends.
Inputs may be any that keep to these rules, and one draw needn't show every extreme that they name: `expert_ids`: each row names 2 different experts. Among the 8 rows of one device no expert is named by more than 4 rows, and on some devices one expert is named by exactly 4 rows. `next_ids`: each row names 2 different experts.
All inputs are finite; a program needn't handle non-finite values.
Results may differ from the reference program's by a relative error of at most 0.013.
Values may be sent and summed in bfloat16 or wider, within the bound.
A program may use at most 128 MiB of HBM per device.

```python
import math
import jax
import jax.numpy as jnp
import numpy as np
from jax import lax

D = 6144
FF = 8192
EXPERTS = 8
TOP = 2
TOK_DEV = 8
CAP = 4
TOKENS = 256


def levels(rng, extent, shards, low, top_value):
    gain, own = 1.0, jax.random.fold_in(rng, 6)
    for position, parts in shards:
        heights = jnp.exp(jax.random.uniform(jax.random.fold_in(own, position), (parts,), jnp.float32, low / len(shards), top_value / len(shards)))
        gain = gain * jnp.repeat(heights, extent[position] // parts).reshape([-1 if axis == position else 1 for axis in range(len(extent))])
    return gain


def picks_of(rng, rows, amount, top, lift):
    order = jax.random.permutation(jax.random.fold_in(rng, 1), amount)
    favour = order
    for power in range(3):
        favour = favour * favour // amount
    favour = favour * lift // amount
    tickets = jax.random.randint(jax.random.fold_in(rng, 2), (rows, amount), 0, 4096) + favour
    fixed_rows = jax.random.permutation(jax.random.fold_in(rng, 3), rows)[jnp.arange(amount) % rows]
    tickets = jnp.where(jnp.arange(rows)[:, None] == fixed_rows[None, :], 1 << 14, tickets)
    score = tickets * amount + jnp.arange(amount)
    return lax.top_k(score.astype(jnp.int32), top)[1].astype(jnp.int32)


def assign_block(stream_key, own, number, rows, amount, top, limit, slope):
    ranking = jax.random.permutation(stream_key, amount)
    packed, usual = portions_of(amount, rows * top, limit, slope, True), portions_of(amount, rows * top, limit, slope, False)
    places = jnp.arange(amount)

    def named(tallies, turn):
        used = int((tallies > 0).sum())
        fixed = max(1, used // 4)
        moved = fixed + (places - fixed + turn * (used - fixed)) % max(1, amount - fixed)
        return jnp.zeros((amount,), jnp.int32).at[ranking[jnp.where(places < fixed, places, moved)]].set(jnp.asarray(tallies, jnp.int32))

    tallies = jnp.where(number % 4 == 0, named(packed, number // 4), named(usual, number - number // 4 - 1))
    mixed = jax.random.permutation(jax.random.fold_in(own, 3), amount)
    donor, receiver = mixed[0:amount // 2 * 2:2], mixed[1:amount // 2 * 2:2]
    slack = jnp.minimum(tallies[donor] - 1, limit - tallies[receiver]) // 2
    slack = jnp.where((donor == ranking[0]) | (receiver == ranking[0]) | (tallies[receiver] == 0), 0, jnp.maximum(slack, 0))
    moved = jax.random.randint(jax.random.fold_in(own, 4), (amount // 2,), 0, 1 << 20) % (slack + 1)
    tallies = tallies.at[donor].add(-moved).at[receiver].add(moved)
    items = jnp.searchsorted(jnp.cumsum(tallies), jnp.arange(rows * top), side="right").astype(jnp.int32)
    listing = items.reshape(top, rows).T
    listing = listing[jax.random.permutation(jax.random.fold_in(own, 1), rows)]
    turn = jax.random.randint(jax.random.fold_in(own, 2), (rows, 1), 0, top)
    return jnp.take_along_axis(listing, (jnp.arange(top)[None, :] + turn) % top, axis=1)


def portions_of(amount, total, most, skew, full):
    weights = [(1 << 20) // math.isqrt(rank ** skew) + 1 for rank in range(1, amount + 1)]
    largest = most if full else min(most, max(-(-total // amount), total * weights[0] // sum(weights)))
    least = 1 if total - largest >= amount - 1 else 0
    counts, rest = [largest] + [least] * (amount - 1), total - largest - least * (amount - 1)
    while rest > 0:
        candidates = [i for i in range(1, amount) if counts[i] < largest] or [i for i in range(1, amount) if counts[i] < most]
        pool, budget = sum([weights[i] for i in candidates]), rest
        for i in candidates:
            more = min(most - counts[i], max(1, budget * weights[i] // pool), rest)
            counts[i] = counts[i] + more
            rest = rest - more
    return np.array(counts)


def normal_values(own_key, extent, width, most, cuts=(), kind=jnp.bfloat16):
    array = width * jax.random.normal(own_key, extent, jnp.float32)
    if cuts:
        array = array * levels(own_key, extent, cuts, -0.22, 0.18)
    return jnp.clip(array, -most, most).astype(kind)


def setup_inputs(seed: int = 0) -> dict:
    streams_of = jax.random.split(jax.random.key(seed), 9)
    tokens = normal_values(streams_of[0], (TOKENS, D), 1.0, 6.0, ((0, 32),))
    router_now = normal_values(streams_of[1], (D, EXPERTS), D ** -0.5, 0.078125, ((0, 16),), jnp.float32)
    router_next = normal_values(streams_of[2], (D, EXPERTS), D ** -0.5, 0.078125, ((0, 16),), jnp.float32)
    w_gate = normal_values(streams_of[3], (EXPERTS, D, FF), D ** -0.5, 0.078125, ((0, 2), (2, 16)))
    w_up = normal_values(streams_of[4], (EXPERTS, D, FF), D ** -0.5, 0.078125, ((0, 2), (2, 16)))
    w_down = normal_values(streams_of[5], (EXPERTS, FF, D), FF ** -0.5, 0.0625, ((0, 2), (1, 16)))
    expert_ids_keys = jax.random.split(jax.random.fold_in(streams_of[6], 1), TOKENS // TOK_DEV)
    expert_ids_turns = jax.random.permutation(jax.random.fold_in(streams_of[6], 3), TOKENS // TOK_DEV)
    expert_ids = jax.vmap(lambda own, number: assign_block(jax.random.fold_in(streams_of[6], 2), own, number, TOK_DEV, EXPERTS, TOP, CAP, 2))(expert_ids_keys, expert_ids_turns).reshape((TOKENS, TOP))
    next_ids = picks_of(streams_of[7], TOKENS, EXPERTS, TOP, 2048)
    return dict(tokens=tokens, router_now=router_now, router_next=router_next, w_gate=w_gate, w_up=w_up, w_down=w_down, expert_ids=expert_ids, next_ids=next_ids)


epsilon = 1e-05

def rms_normed(values):
    return values * lax.rsqrt(lax.optimization_barrier(jnp.mean(values * values, axis=-1, keepdims=True)) + epsilon)

def pair_weights(logits, chosen):
    picked = jnp.take_along_axis(logits, chosen, axis=1)
    first = jax.nn.sigmoid(picked[:, 0] - picked[:, 1])
    return jnp.stack([first, 1.0 - first], axis=1)

def reference(tokens, router_now, router_next, w_gate, w_up, w_down, expert_ids, next_ids):
    resid = tokens.astype(jnp.float32)
    normed = rms_normed(resid)
    logits = jnp.dot(normed, router_now, precision=lax.Precision.HIGHEST, preferred_element_type=jnp.float32)
    weights = pair_weights(logits, expert_ids)
    rounded = normed.astype(jnp.bfloat16)
    blocks = TOKENS // TOK_DEV
    flat = expert_ids.reshape(blocks, TOK_DEV * TOP)
    onehot = (flat[:, :, None] == jnp.arange(EXPERTS, dtype=jnp.int32)[None, None, :]).astype(jnp.int32)
    ranks = lax.optimization_barrier(jnp.sum((jnp.cumsum(onehot, axis=1) - onehot) * onehot, axis=2)).reshape(TOKENS, TOP).astype(jnp.int32)
    block_of = jnp.broadcast_to((jnp.arange(TOKENS, dtype=jnp.int32) // TOK_DEV)[:, None], (TOKENS, TOP)).astype(jnp.int32)
    buffer = jnp.zeros((blocks, EXPERTS, CAP, D), jnp.bfloat16)
    buffer = buffer.at[block_of, expert_ids, ranks].set(jnp.broadcast_to(rounded[:, None, :], (TOKENS, TOP, D)))
    rows_in = jnp.transpose(buffer, (1, 0, 2, 3)).reshape(EXPERTS, blocks * CAP, D)

    def expert_out(operands):
        inputs, gate_w, up_w, down_w = operands
        gate = jnp.dot(inputs, gate_w, preferred_element_type=jnp.float32)
        upward = jnp.dot(inputs, up_w, preferred_element_type=jnp.float32)
        hidden = (jax.nn.silu(gate) * upward).astype(jnp.bfloat16)
        return jnp.dot(hidden, down_w, preferred_element_type=jnp.float32)
    outputs = lax.map(expert_out, (rows_in, w_gate, w_up, w_down)).reshape(EXPERTS, blocks, CAP, D)
    picked = outputs[expert_ids, block_of, ranks]
    mixture = lax.optimization_barrier(jnp.sum(picked * weights[:, :, None], axis=1))
    summed = resid + mixture
    layer_out = summed.astype(jnp.bfloat16)
    next_logits = jnp.dot(rms_normed(summed), router_next, precision=lax.Precision.HIGHEST, preferred_element_type=jnp.float32)
    next_weights = pair_weights(next_logits, next_ids)
    return (layer_out, next_logits, next_weights)
```

```python
import functools

import jax
import jax.numpy as jnp
from jax import lax
from jax.experimental import pallas as pl
from jax.experimental.pallas import tpu as pltpu
from jax.sharding import PartitionSpec as P

epsilon = 1e-05
BOTH = ("dp", "expert")
ROOM = 1 << 21


def rms_normed(values):
    return values * lax.rsqrt(jnp.mean(values * values, axis=-1, keepdims=True) + epsilon)


def pair_weights(logits, chosen):
    picked = jnp.take_along_axis(logits, chosen, axis=1)
    first = jax.nn.sigmoid(picked[:, 0] - picked[:, 1])
    return jnp.stack([first, 1.0 - first], axis=1)


def ffn_kernel(
    in_slots, out_slots, columns, x_ref, share_ref, gate_hbm, up_hbm, down_hbm, out_ref,
    in_buf, down_buf, hidden, in_sem, down_sem,
):
    experts, width, units = gate_hbm.shape
    chunks = width // columns

    def in_copies(e):
        slot = lax.rem(e, in_slots)
        return [
            pltpu.make_async_copy(w.at[e], in_buf.at[slot, i], in_sem.at[slot, i])
            for i, w in enumerate((gate_hbm, up_hbm))
        ]

    def down_copy(n):
        slot = lax.rem(n, out_slots)
        at = pl.ds(pl.multiple_of(n * columns, 128), columns)
        return pltpu.make_async_copy(
            down_hbm.at[:, :, at], down_buf.at[slot], down_sem.at[slot]
        )

    for e in range(min(in_slots, experts)):
        for copy in in_copies(e):
            copy.start()
    for n in range(min(out_slots, chunks)):
        down_copy(n).start()

    def first(e, carry):
        slot = lax.rem(e, in_slots)
        gate_copy, up_copy = in_copies(e)
        gate_copy.wait()
        gate = jnp.dot(x_ref[...], in_buf[slot, 0], preferred_element_type=jnp.float32)
        up_copy.wait()
        upward = jnp.dot(x_ref[...], in_buf[slot, 1], preferred_element_type=jnp.float32)
        value = gate / (1.0 + jnp.exp(-gate)) * upward * share_ref[e]
        hidden[:, pl.ds(pl.multiple_of(e * units, 128), units)] = value.astype(jnp.bfloat16)

        @pl.when(e + in_slots < experts)
        def _():
            for copy in in_copies(e + in_slots):
                copy.start()

        return carry

    lax.fori_loop(0, experts, first, 0)

    def second(n, carry):
        slot = lax.rem(n, out_slots)
        down_copy(n).wait()
        weights = down_buf[slot].reshape(experts * units, columns)
        total = jnp.dot(hidden[...], weights, preferred_element_type=jnp.float32)
        out_ref[:, pl.ds(pl.multiple_of(n * columns, 128), columns)] = total.astype(jnp.bfloat16)

        @pl.when(n + out_slots < chunks)
        def _():
            down_copy(n + out_slots).start()

        return carry

    lax.fori_loop(0, chunks, second, 0)


def local_experts(everyone, share, w_gate, w_up, w_down):
    experts, width, units = w_gate.shape
    rows = everyone.shape[0]
    if rows * width > ROOM:
        total = jnp.zeros((rows, width), jnp.float32)
        for e in range(experts):
            gate = jnp.dot(everyone, w_gate[e], preferred_element_type=jnp.float32)
            upward = jnp.dot(everyone, w_up[e], preferred_element_type=jnp.float32)
            value = gate / (1.0 + jnp.exp(-gate)) * upward * share[e]
            value = value.astype(jnp.bfloat16)
            total = total + jnp.dot(value, w_down[e], preferred_element_type=jnp.float32)
        return total.astype(jnp.bfloat16)
    columns, in_slots, out_slots = 768, 3, 4
    vmem = pl.BlockSpec(memory_space=pltpu.VMEM)
    hbm = pl.BlockSpec(memory_space=pltpu.HBM)
    return pl.pallas_call(
        functools.partial(ffn_kernel, in_slots, out_slots, columns),
        out_shape=jax.ShapeDtypeStruct((rows, width), jnp.bfloat16),
        in_specs=[vmem, vmem, hbm, hbm, hbm],
        out_specs=vmem,
        scratch_shapes=[
            pltpu.VMEM((in_slots, 2, width, units), jnp.bfloat16),
            pltpu.VMEM((out_slots, experts, units, columns), jnp.bfloat16),
            pltpu.VMEM((rows, experts * units), jnp.bfloat16),
            pltpu.SemaphoreType.DMA((in_slots, 2)),
            pltpu.SemaphoreType.DMA((out_slots,)),
        ],
        compiler_params=pltpu.CompilerParams(vmem_limit_bytes=67043328),
        cost_estimate=pl.CostEstimate(
            flops=6 * rows * experts * width * units,
            bytes_accessed=6 * experts * width * units,
            transcendentals=0,
        ),
    )(everyone, share, w_gate, w_up, w_down)


def on_device(tokens, router_now, router_next, w_gate, w_up, w_down, expert_ids, next_ids):
    experts, width, units = w_gate.shape
    count = router_now.shape[1]
    resid = tokens.astype(jnp.float32)
    normed = rms_normed(resid)
    everyone = lax.all_gather(normed.astype(jnp.bfloat16), BOTH, axis=0, tiled=True)
    rows = everyone.shape[0]
    routers = jnp.concatenate([router_now.T, router_next.T], axis=0)
    routers = lax.all_gather(routers, "dp", axis=1, tiled=True)
    whole_now, whole_next = routers[:count], routers[count:]
    exact = functools.partial(
        lax.dot_general,
        dimension_numbers=(((1,), (1,)), ((), ())),
        precision=lax.Precision.HIGHEST,
        preferred_element_type=jnp.float32,
    )
    logits = exact(normed, whole_now)
    weights = pair_weights(logits, expert_ids)
    named = expert_ids[:, :, None] == jnp.arange(count, dtype=jnp.int32)[None, None, :]
    table = jnp.sum(jnp.where(named, weights[:, :, None], 0.0), axis=1)
    table = lax.all_gather(table, BOTH, axis=0, tiled=True)
    share = lax.dynamic_slice_in_dim(table, lax.axis_index("expert") * experts, experts, axis=1)
    share = share.T[:, :, None]

    partial = local_experts(everyone, share, w_gate, w_up, w_down)
    mixture = lax.psum_scatter(partial, BOTH, scatter_dimension=0, tiled=True)
    summed = resid + mixture.astype(jnp.float32)
    layer_out = summed.astype(jnp.bfloat16)
    next_logits = exact(rms_normed(summed), whole_next)
    return (layer_out, next_logits, pair_weights(next_logits, next_ids))


def solution(mesh):
    in_specs = (
        P(BOTH, None),
        P("dp", None),
        P("dp", None),
        P("expert", None, "dp"),
        P("expert", None, "dp"),
        P("expert", "dp", None),
        P(BOTH, None),
        P(BOTH, None),
    )
    out_specs = (P(BOTH, None), P(BOTH, None), P(BOTH, None))
    return jax.shard_map(
        on_device, mesh=mesh, in_specs=in_specs, out_specs=out_specs, check_vma=False
    )
```
